512 devices in a mesh: groups: 2 (over y), batch: 16 (over z), blk: 16 (over x, core).
Axes of the slice: x: 8, y: 2, z: 16, core: 2. Of those that a mesh axis runs over, the one named last changes fastest.
The devices are a block of a 8x8x16 slice.
Arguments:
- queries: bfloat16 [32, 2368, 1024], P(('groups', 'batch'), 'blk'), parts along dimension 0, may hold values from -12 to 12
- key_states: bfloat16 [32, 2368, 1024], P(('groups', 'batch'), 'blk'), parts along dimension 0, may hold values from -6 to 6
- value_states: bfloat16 [32, 2368, 1024], P(('groups', 'batch'), 'blk'), parts along dimension 0, may hold values from -6 to 6
- residual: bfloat16 [32, 2368, 768], P(('groups', 'batch'), 'blk'), parts along dimension 0, may hold values from -3 to 3
- proj_weight: bfloat16 [1024, 768], P(None, 'batch'), may hold values from -0.1875 to 0.1875
- conv_weight: bfloat16 [3, 3, 768, 384], P(None, None, 'batch'), may hold values from -0.078125 to 0.078125
Outputs:
- conv_out: bfloat16 [32, 2368, 384], P(('groups', 'batch'), 'blk'), parts along dimension 0
The draws below stay inside these ranges and needn't reach their ends.
There are 2 independent parts, one for each index of `groups`. The reference program is written for one: setup_inputs(seed, part) draws one part's arguments, and reference() takes and returns one part's arrays. A program takes and returns all parts, laid end to end along the dimension named above; an argument that names none is the same for every part. Nothing has to cross between parts.
All inputs are finite; a program needn't handle non-finite values.
Results may differ from the reference program's by a relative error of at most 0.0085.
Values may be sent and summed in bfloat16 or wider, within the bound.
A program may use at most 64 MiB of HBM per device.

```python
import jax
import jax.numpy as jnp
from jax import lax

HEADS = 16
HD = 64
FEATW = 768
FEAT = 384
COLS = 74
NROWS = 32
TOKENS = 2368
IMAGES = 16


def draw_queries(key, part):
    base_draw = 3.0 * jnp.clip(jax.random.normal(jax.random.fold_in(key, 1), (IMAGES, TOKENS, HEADS * HD), jnp.float32), -4.0, 4.0)
    return base_draw.astype(jnp.bfloat16)


def draw_key_states(key, part):
    base_draw = jnp.clip(jax.random.normal(jax.random.fold_in(key, 2), (IMAGES, TOKENS, HEADS * HD), jnp.float32), -6.0, 6.0)
    return base_draw.astype(jnp.bfloat16)


def levels(key, shape, shards, low, largest):
    level, own = 1.0, jax.random.fold_in(key, 6)
    for position, blocks in shards:
        steps = jnp.exp(jax.random.uniform(jax.random.fold_in(own, position), (blocks,), jnp.float32, low / len(shards), largest / len(shards)))
        level = level * jnp.repeat(steps, shape[position] // blocks).reshape([-1 if axis == position else 1 for axis in range(len(shape))])
    return level


def gaussian(rng, dims, deviation, bound, pieces=(), kind=jnp.bfloat16):
    result = jax.random.normal(rng, dims, jnp.float32) * deviation
    if len(pieces) > 0:
        result = levels(rng, dims, pieces, -0.22, 0.18) * result
    return jnp.clip(result, min=-bound, max=bound).astype(kind)


def setup_inputs(seed: int = 0, part: int = 0) -> dict:
    key_of = jax.random.split(jax.random.key(seed), 7)
    part_keys = jax.random.split(jax.random.fold_in(key_of[6], part), 7)
    queries = draw_queries(jax.random.fold_in(jax.random.fold_in(key_of[6], part), 71), part)
    key_states = draw_key_states(jax.random.fold_in(jax.random.fold_in(key_of[6], part), 71), part)
    value_states = gaussian(part_keys[2], (IMAGES, TOKENS, HEADS * HD), 1.0, 6.0, ((0, 16), (1, 16)))
    residual = gaussian(part_keys[3], (IMAGES, TOKENS, FEATW), 0.5, 3.0, ((0, 16), (1, 16)))
    proj_weight = gaussian(key_of[4], (HEADS * HD, FEATW), (HEADS * HD) ** -0.5, 0.1875, ((1, 16),))
    conv_weight = gaussian(key_of[5], (3, 3, FEATW, FEAT), (9 * FEATW) ** -0.5, 0.078125, ((2, 16),))
    return dict(queries=queries, key_states=key_states, value_states=value_states, residual=residual, proj_weight=proj_weight, conv_weight=conv_weight)


def one_head(head_args):
    query_head, key_head, value_head = head_args
    scores = jnp.dot(query_head, key_head.T, preferred_element_type=jnp.float32) * (HD ** -0.5)
    row_max = jnp.max(scores, axis=1, keepdims=True)
    weights = jnp.exp(scores - row_max)
    weight_sum = jnp.sum(weights, axis=1, keepdims=True)
    mixed = jnp.dot(weights.astype(jnp.bfloat16), value_head, preferred_element_type=jnp.float32)
    return mixed / weight_sum


def one_image(image_args, proj_weight, conv_weight):
    queries, key_states, value_states, residual = image_args
    query_heads = queries.reshape(TOKENS, HEADS, HD).transpose(1, 0, 2)
    key_heads = key_states.reshape(TOKENS, HEADS, HD).transpose(1, 0, 2)
    value_heads = value_states.reshape(TOKENS, HEADS, HD).transpose(1, 0, 2)
    mixed = lax.map(one_head, (query_heads, key_heads, value_heads))
    attention = mixed.transpose(1, 0, 2).reshape(TOKENS, HEADS * HD).astype(jnp.bfloat16)
    projected = jnp.dot(attention, proj_weight, preferred_element_type=jnp.float32)
    hidden = (residual.astype(jnp.float32) + projected).astype(jnp.bfloat16)
    feature_grid = hidden.reshape(NROWS, COLS, FEATW)
    padded = jnp.pad(feature_grid, ((1, 1), (1, 1), (0, 0)))
    conv_sum = jnp.zeros((TOKENS, FEAT), jnp.float32)
    for row_off in range(3):
        for col_off in range(3):
            window = padded[row_off:row_off + NROWS, col_off:col_off + COLS].reshape(TOKENS, FEATW)
            conv_sum = conv_sum + jnp.dot(window, conv_weight[row_off, col_off], preferred_element_type=jnp.float32)
    return conv_sum.astype(jnp.bfloat16)


def reference(queries, key_states, value_states, residual, proj_weight, conv_weight):
    return lax.map(lambda image_args: one_image(image_args, proj_weight, conv_weight),
                   (queries, key_states, value_states, residual))
```

```python
import functools

import jax
import jax.numpy as jnp
from jax import lax
from jax.experimental import pallas as pl
from jax.experimental.pallas import tpu as pltpu
from jax.sharding import PartitionSpec as P

HD = 64
COLS = 74
ROWS = 2
LANES = 128
LOG2E = 1.4426950408889634
MESH = pl.DeviceIdType.MESH
F32 = jnp.float32
BF16 = jnp.bfloat16
NT = (((1,), (1,)), ((), ()))


def up16(n):
    return -(-n // 16) * 16


def one_hot(rows, depth, dc, pitch, flag):
    i = lax.broadcasted_iota(jnp.int32, (rows, depth), 0)
    t = lax.broadcasted_iota(jnp.int32, (rows, depth), 1)
    r = jnp.where(i >= pitch, 1, 0)
    c = i - r * pitch
    src = c + (dc - 1)
    ok = (t == r * COLS + src) & (c < COLS) & (src >= 0) & (src < COLS)
    if flag is not None:
        ok = ok & flag
    return jnp.where(ok, 1.0, 0.0).astype(BF16)


def kernel(dims, q, k, v, res, w, out, kin, vin, qin, ob, ain, wall, kpad, vaug, qpad,
           hpad, grid, hin, rbuf, k_s, k_r, v_s, v_r, q_s, q_r, o_s, o_r, kf_s, kf_r,
           vf_s, vf_r, w_s, w_r, p_s, p_r, h_s, h_r, loc):
    nb, nz, tok, slab, taps, pitch, cp = dims
    xn = nb // 2
    half = taps // 2
    blk = lax.axis_index("blk")
    z = lax.axis_index("batch")
    x = blk // 2
    c = blk % 2
    mate = 2 * x + 1 - c
    side = lax.rem(blk + nb + 2 * c - 1, nb)
    znext = (lax.rem(z + 1, nz), lax.rem(z + nz - 1, nz))
    hops = (nz // 2, nz - 1 - nz // 2)

    def at_x(i):
        off = ((i + 1) // 2) * (2 * (i % 2) - 1)
        return lax.rem(x + off + xn, xn)

    def wait(ref, sem):
        pltpu.make_async_copy(ref, ref, sem).wait()

    def send(src, dst, s_sem, r_sem, **where):
        pltpu.make_async_remote_copy(
            src_ref=src, dst_ref=dst, send_sem=s_sem, recv_sem=r_sem,
            device_id=where, device_id_type=MESH,
        ).start()

    barrier = pltpu.get_barrier_semaphore()
    for i in range(1, xn):
        pl.semaphore_signal(barrier, inc=1, device_id={"blk": 2 * at_x(i) + c}, device_id_type=MESH)
    for b in (mate, side):
        pl.semaphore_signal(barrier, inc=1, device_id={"blk": b}, device_id_type=MESH)
    for n in znext:
        pl.semaphore_signal(barrier, inc=1, device_id={"batch": n}, device_id_type=MESH)
    pl.semaphore_wait(barrier, xn - 1 + 4)

    def cols(i):
        return pl.ds(pl.multiple_of(i * LANES, LANES), LANES)

    def slab_rows(zz):
        return pl.ds(pl.multiple_of(zz * slab, slab), slab)

    for i in range(1, xn):
        d = at_x(i)
        send(k.at[0, :, cols(d)], kin.at[c, x], k_s.at[i], k_r.at[x], blk=2 * d + c)
        send(v.at[0, :, cols(d)], vin.at[c, x], v_s.at[i], v_r.at[x], blk=2 * d + c)
        if i == 2:
            for j in range(half):
                for way in range(2):
                    send(w.at[half * c + j], wall.at[half * c + j, slab_rows(z)],
                         w_s.at[way, j], w_r.at[way, 0, j], batch=znext[way])
    for i in range(1, xn):
        d = at_x(i)
        send(q.at[0, :, cols(d)], qin.at[x], q_s.at[i], q_r.at[x], blk=2 * d + c)
    pltpu.make_async_copy(k.at[0, :, cols(x)], kin.at[c, x], k_r.at[x]).start()
    pltpu.make_async_copy(v.at[0, :, cols(x)], vin.at[c, x], v_r.at[x]).start()
    pltpu.make_async_copy(q.at[0, :, cols(x)], qin.at[x], q_r.at[x]).start()
    pltpu.make_async_copy(w, wall.at[:, slab_rows(z)], loc.at[0]).start()
    pltpu.make_async_copy(res.at[0], rbuf, loc.at[1]).start()

    def tick(t, carry):
        s = t // half
        j = lax.rem(t, half)
        for way in range(2):
            zz = lax.rem(z + (1 + s if way else 2 * nz - 1 - s), nz)

            def work():
                ref = wall.at[half * c + j, slab_rows(zz)]
                wait(ref, w_r.at[way, s, j])

                @pl.when(s < hops[way] - 1)
                def _():
                    wait(ref, w_s.at[way, j])
                    send(ref, ref, w_s.at[way, j], w_r.at[way, s + 1, j], batch=znext[way])

                @pl.when(s > 0)
                def _():
                    wait(ref, p_s.at[way, j])

                send(ref, ref, p_s.at[way, j], p_r.at[way, s, j], blk=mate)

            if hops[way] == hops[0]:
                work()
            else:
                pl.when(s < hops[way])(work)
        return carry

    def ticks(lo, hi):
        lax.fori_loop(lo, hi, tick, 0)

    kpad[...] = jnp.zeros_like(kpad)
    vaug[...] = jnp.zeros_like(vaug)
    qpad[...] = jnp.zeros_like(qpad)
    hpad[...] = jnp.zeros_like(hpad)

    tail = tok // 16 * 16

    def place(p, xs):
        base = (p * xn + xs) * pitch
        kpad[pl.ds(pl.multiple_of(base, 16), tok), :] = kin[p, xs]
        last = kpad[pl.ds(pl.multiple_of(base + tail, 16), 16), :].astype(F32)
        prior = kpad[pl.ds(pl.multiple_of(base + tail - 16, 16), 16), :].astype(F32)
        row = lax.broadcasted_iota(jnp.int32, (16, LANES), 0)
        kpad[pl.ds(pl.multiple_of(base + tail, 16), 16), :] = jnp.where(
            row < tok - tail, last, prior).astype(BF16)
        vaug[pl.ds(pl.multiple_of(base, 16), tok), 0:LANES] = vin[p, xs]
        vaug[pl.ds(pl.multiple_of(base, 16), tok), LANES:2 * LANES] = jnp.ones((tok, LANES), BF16)

    def take(i, carry):
        xs = at_x(i)
        wait(kin.at[c, xs], k_r.at[xs])
        send(kin.at[c, xs], kin.at[c, xs], kf_s.at[xs], kf_r.at[xs], blk=mate)
        wait(vin.at[c, xs], v_r.at[xs])
        send(vin.at[c, xs], vin.at[c, xs], vf_s.at[xs], vf_r.at[xs], blk=mate)
        place(c, xs)
        lax.fori_loop(2 * i, 2 * i + 2, tick, 0)
        return carry

    lax.fori_loop(0, xn, take, 0)

    def take_mate(i, carry):
        xs = at_x(i)
        wait(kin.at[1 - c, xs], kf_r.at[xs])
        wait(vin.at[1 - c, xs], vf_r.at[xs])
        place(1 - c, xs)
        return carry

    lax.fori_loop(0, xn, take_mate, 0)

    lane = lax.broadcasted_iota(jnp.int32, (tok, LANES), 1)
    scale = HD ** -0.5 * LOG2E

    def attend(i, carry):
        xs = at_x(i)
        wait(qin.at[xs], q_r.at[xs])
        qv = qin[xs].astype(F32)
        qpad[0:tok, :] = jnp.where(lane < HD, qv, 0.0).astype(BF16)
        qpad[pitch:pitch + tok, :] = jnp.where(lane < HD, 0.0, qv).astype(BF16)
        scores = lax.dot_general(qpad[...], kpad[...], NT, preferred_element_type=F32)
        top = jnp.max(scores, axis=1, keepdims=True)
        weights = jnp.exp2((scores - top) * scale).astype(BF16)
        mixed = jnp.dot(weights, vaug[...], preferred_element_type=F32)
        both = mixed[:, :LANES] / mixed[:, LANES:]
        ob[xs] = jnp.where(lane < HD, both[0:tok], both[pitch:pitch + tok]).astype(BF16)

        @pl.when(i == 0)
        def _():
            ain[x] = ob[x]

        @pl.when(i > 0)
        def _():
            send(ob.at[xs], ain.at[x], o_s.at[xs], o_r.at[x], blk=2 * xs + c)

        lax.fori_loop(2 * xn + 2 * i, 2 * xn + 2 * i + 2, tick, 0)
        return carry

    lax.fori_loop(0, xn, attend, 0)
    ticks(4 * xn, hops[0] * half)

    for way in range(2):
        for s in range(hops[way]):
            zz = lax.rem(z + (1 + s if way else 2 * nz - 1 - s), nz)
            for j in range(half):
                wait(wall.at[half * (1 - c) + j, slab_rows(zz)], p_r.at[way, s, j])
    wait(wall.at[:, slab_rows(z)], loc.at[0])
    wait(rbuf, loc.at[1])
    for i in range(1, xn):
        xs = at_x(i)
        wait(ain.at[xs], o_r.at[xs])

    attention = jnp.concatenate([ain[i] for i in range(xn)], axis=1)
    width = wall.shape[2]
    total = rbuf[...].astype(F32)
    convs = taps - (-(-attention.shape[1] // width))
    for b in range(convs, taps):
        lo = (b - convs) * width
        hi = min(lo + width, attention.shape[1])
        total = total + lax.dot_general(
            attention[:, lo:hi], wall[b, :, 0:hi - lo], NT, preferred_element_type=F32)
    hpad[0:tok, :] = total.astype(BF16)

    hid = hpad[...]
    for dc in (1, 0, 2):
        grid[dc, cp:3 * cp, :] = jnp.dot(
            one_hot(2 * cp, pitch, dc, cp, None), hid, preferred_element_type=F32).astype(BF16)
        if dc == 1:
            send(grid.at[1, cp:2 * cp], hin.at[1], h_s.at[0], h_r.at[1],
                 blk=lax.rem(blk + nb - 1, nb))
            send(grid.at[1, 2 * cp:3 * cp], hin.at[0], h_s.at[1], h_r.at[0],
                 blk=lax.rem(blk + 1, nb))

    both_rows = jnp.zeros((2 * cp, out.shape[1]), F32)
    for dc in range(3):
        both_rows += jnp.dot(grid[dc, cp:3 * cp, :], wall[3 + dc], preferred_element_type=F32)
    upper = both_rows[0:cp]
    lower = both_rows[cp:2 * cp]
    for dc in range(3):
        upper += jnp.dot(grid[dc, 2 * cp:3 * cp, :], wall[6 + dc], preferred_element_type=F32)
        lower += jnp.dot(grid[dc, cp:2 * cp, :], wall[dc], preferred_element_type=F32)
    wait(hin.at[0], h_r.at[0])
    wait(hin.at[1], h_r.at[1])
    for dc in range(3):
        above = jnp.dot(one_hot(cp, cp, dc, cp, blk > 0), hin[0], preferred_element_type=F32)
        below = jnp.dot(one_hot(cp, cp, dc, cp, blk < nb - 1), hin[1], preferred_element_type=F32)
        upper += jnp.dot(above.astype(BF16), wall[dc], preferred_element_type=F32)
        lower += jnp.dot(below.astype(BF16), wall[6 + dc], preferred_element_type=F32)
    out[0:cp, :] = upper.astype(BF16)
    out[cp:2 * cp, :] = lower.astype(BF16)

    for i in range(1, xn):
        xs = at_x(i)
        wait(kin.at[c, 0], k_s.at[i])
        wait(vin.at[c, 0], v_s.at[i])
        wait(qin.at[0], q_s.at[i])
        wait(ob.at[xs], o_s.at[xs])
    for i in range(xn):
        wait(kin.at[c, i], kf_s.at[i])
        wait(vin.at[c, i], vf_s.at[i])
    for way in range(2):
        for j in range(half):
            wait(wall.at[j, slab_rows(z)], w_s.at[way, j])
            wait(wall.at[j, slab_rows(z)], p_s.at[way, j])
    wait(hin.at[0], h_s.at[0])
    wait(hin.at[1], h_s.at[1])


def body(queries, key_states, value_states, residual, proj_weight, conv_weight):
    nb = lax.axis_size("blk")
    nz = lax.axis_size("batch")
    tok = queries.shape[1]
    slab = conv_weight.shape[2]
    width = conv_weight.shape[3]
    depth = proj_weight.shape[0]
    blocks = -(-depth // width)
    flat = jnp.pad(proj_weight, ((0, blocks * width - depth), (0, 0)))
    flat = flat.reshape(blocks, width, slab).transpose(0, 2, 1)
    weights = jnp.concatenate([conv_weight.reshape(9, slab, width), flat], axis=0)
    taps = weights.shape[0]
    half = taps // 2
    xn = nb // 2
    pitch = up16(tok)
    cp = up16(COLS)
    feats = nz * slab
    hops = nz // 2
    dma = pltpu.SemaphoreType.DMA
    any_space = pl.BlockSpec(memory_space=pl.ANY)
    got = pl.pallas_call(
        functools.partial(kernel, (nb, nz, tok, slab, taps, pitch, cp)),
        out_shape=jax.ShapeDtypeStruct((2 * cp, width), BF16),
        in_specs=[any_space] * 5,
        out_specs=pl.BlockSpec(memory_space=pltpu.VMEM),
        scratch_shapes=[
            pltpu.VMEM((2, xn, tok, LANES), BF16),
            pltpu.VMEM((2, xn, tok, LANES), BF16),
            pltpu.VMEM((xn, tok, LANES), BF16),
            pltpu.VMEM((xn, tok, LANES), BF16),
            pltpu.VMEM((xn, tok, LANES), BF16),
            pltpu.VMEM((taps, feats, width), BF16),
            pltpu.VMEM((nb * pitch, LANES), BF16),
            pltpu.VMEM((nb * pitch, 2 * LANES), BF16),
            pltpu.VMEM((2 * pitch, LANES), BF16),
            pltpu.VMEM((pitch, feats), BF16),
            pltpu.VMEM((3, 4 * cp, feats), BF16),
            pltpu.VMEM((2, cp, feats), BF16),
            pltpu.VMEM((tok, feats), BF16),
            dma((xn,)), dma((xn,)), dma((xn,)), dma((xn,)), dma((xn,)), dma((xn,)),
            dma((xn,)), dma((xn,)), dma((xn,)), dma((xn,)), dma((xn,)), dma((xn,)),
            dma((2, half)), dma((2, hops, half)), dma((2, half)), dma((2, hops, half)),
            dma((2,)), dma((2,)), dma((2,)),
        ],
        compiler_params=pltpu.CompilerParams(
            collective_id=0, has_side_effects=True, vmem_limit_bytes=60 * 1024 * 1024),
    )(queries, key_states, value_states, residual, weights)
    return got.reshape(ROWS, cp, width)[:, :COLS].reshape(1, tok, width)


def solution(mesh):
    return jax.shard_map(
        body,
        mesh=mesh,
        in_specs=(
            P(("groups", "batch"), "blk", None),
            P(("groups", "batch"), "blk", None),
            P(("groups", "batch"), "blk", None),
            P(("groups", "batch"), "blk", None),
            P(None, "batch"),
            P(None, None, "batch", None),
        ),
        out_specs=P(("groups", "batch"), "blk", None),
        check_vma=False,
    )
```

```python
import functools

import jax
import jax.numpy as jnp
from jax import lax
from jax.experimental import pallas as pl
from jax.experimental.pallas import tpu as pltpu
from jax.sharding import PartitionSpec as P

HD = 64
COLS = 74
ROWS = 2
LANES = 128
LOG2E = 1.4426950408889634
MESH = pl.DeviceIdType.MESH
F32 = jnp.float32
BF16 = jnp.bfloat16
NT = (((1,), (1,)), ((), ()))


def up16(n):
    return -(-n // 16) * 16


def one_hot(rows, depth, dc, pitch, flag):
    i = lax.broadcasted_iota(jnp.int32, (rows, depth), 0)
    t = lax.broadcasted_iota(jnp.int32, (rows, depth), 1)
    r = jnp.where(i >= pitch, 1, 0)
    c = i - r * pitch
    src = c + (dc - 1)
    ok = (t == r * COLS + src) & (c < COLS) & (src >= 0) & (src < COLS)
    if flag is not None:
        ok = ok & flag
    return jnp.where(ok, 1.0, 0.0).astype(BF16)


def kernel(dims, q, k, v, res, conv, proj, out, kin, vin, qin, ob, ain, wall, kpad, vaug, qpad,
           hpad, grid, hin, rbuf, k_s, k_r, v_s, v_r, q_s, q_r, o_s, o_r, kf_s, kf_r,
           vf_s, vf_r, w_s, w_r, p_s, p_r, h_s, h_r, loc, go, flat):
    nb, nz, tok, slab, taps, pitch, cp, hops = dims
    xn = nb // 2
    parts = taps // 3
    blk = lax.axis_index("blk")
    z = lax.axis_index("batch")
    x = blk // 2
    c = blk % 2
    mate = 2 * x + 1 - c
    side = lax.rem(blk + nb + 2 * c - 1, nb)
    znext = (lax.rem(z + 1, nz), lax.rem(z + nz - 1, nz))

    def at_x(i):
        off = ((i + 1) // 2) * (2 * (i % 2) - 1)
        return lax.rem(x + off + xn, xn)

    def wait(ref, sem):
        pltpu.make_async_copy(ref, ref, sem).wait()

    def send(src, dst, s_sem, r_sem, **where):
        pltpu.make_async_remote_copy(
            src_ref=src, dst_ref=dst, send_sem=s_sem, recv_sem=r_sem,
            device_id=where, device_id_type=MESH,
        ).start()

    barrier = pltpu.get_barrier_semaphore()
    for i in range(xn):
        d = at_x(i)
        if i > 0:
            pl.semaphore_signal(barrier, inc=1, device_id={"blk": 2 * d}, device_id_type=MESH)
        else:
            @pl.when(c == 1)
            def _():
                pl.semaphore_signal(barrier, inc=1, device_id={"blk": mate}, device_id_type=MESH)

    @pl.when(c == 1)
    def _():
        for n in znext:
            pl.semaphore_signal(barrier, inc=1, device_id={"batch": n}, device_id_type=MESH)

    @pl.when(c == 0)
    def _():
        pl.semaphore_wait(barrier, nb - 1)
        pl.semaphore_signal(go, inc=1, device_id={"blk": mate}, device_id_type=MESH)

    @pl.when(c == 1)
    def _():
        pl.semaphore_wait(go, 1)

    def cols(i):
        return pl.ds(pl.multiple_of(i * LANES, LANES), LANES)

    def slab_rows(zz):
        return pl.ds(pl.multiple_of(zz * slab, slab), slab)

    for i in range(1, xn):
        d = at_x(i)
        send(k.at[0, :, cols(d)], kin.at[c, x], k_s.at[i], k_r.at[x], blk=2 * d + c)
        send(v.at[0, :, cols(d)], vin.at[c, x], v_s.at[i], v_r.at[x], blk=2 * d + c)
    for i in range(1, xn):
        d = at_x(i)
        send(q.at[0, :, cols(d)], qin.at[x], q_s.at[i], q_r.at[x], blk=2 * d + c)
    pltpu.make_async_copy(k.at[0, :, cols(x)], kin.at[c, x], k_r.at[x]).start()
    pltpu.make_async_copy(v.at[0, :, cols(x)], vin.at[c, x], v_r.at[x]).start()
    pltpu.make_async_copy(q.at[0, :, cols(x)], qin.at[x], q_r.at[x]).start()
    pltpu.make_async_copy(conv, wall.at[0:9, slab_rows(z)], loc.at[0]).start()
    pltpu.make_async_copy(res.at[0], rbuf, loc.at[1]).start()

    def part(j):
        return pl.ds(3 * lax.rem(j + parts - 1, parts), 3)

    width = wall.shape[2]
    depth = proj.shape[0]
    for b in range(taps - 9):
        n = min(width, depth - b * width)
        turned = proj[b * width:b * width + n, :].astype(F32).T.astype(BF16)
        flat[b, :, 0:n] = turned
        if n < width:
            flat[b, :, n:width] = jnp.zeros((slab, width - n), BF16)
        wall[9 + b, slab_rows(z), :] = flat[b]

    @pl.when(c == 1)
    def _():
        pl.semaphore_wait(barrier, 2)
        for j in range(parts):
            first = 3 * ((j + parts - 1) % parts)
            src = flat if first == 9 else conv.at[first:first + 3]
            for way in range(2):
                send(src, wall.at[part(j), slab_rows(z)], w_s.at[way, j], w_r.at[way, 0, j],
                     batch=znext[way])

    def tick(t, carry):
        s = t // parts
        j = lax.rem(t, parts)
        for way in range(2):
            zz = lax.rem(z + (1 + s if way else 2 * nz - 1 - s), nz)

            def work():
                ref = wall.at[part(j), slab_rows(zz)]
                wait(ref, w_r.at[way, s, j])

                @pl.when(s < hops[way] - 1)
                def _():
                    wait(ref, w_s.at[way, j])
                    send(ref, ref, w_s.at[way, j], w_r.at[way, s + 1, j], batch=znext[way])

                @pl.when(s > 0)
                def _():
                    wait(ref, p_s.at[way, j])

                send(ref, ref, p_s.at[way, j], p_r.at[way, s, j], blk=mate)

            if hops[way] == max(hops):
                work()
            else:
                pl.when(s < hops[way])(work)
        return carry

    def ticks(lo, hi):
        @pl.when(c == 1)
        def _():
            lax.fori_loop(lo, hi, tick, 0)

    kpad[...] = jnp.zeros_like(kpad)
    vaug[...] = jnp.zeros_like(vaug)
    qpad[...] = jnp.zeros_like(qpad)
    hpad[...] = jnp.zeros_like(hpad)

    tail = tok // 16 * 16

    def place(p, xs):
        base = (p * xn + xs) * pitch
        kpad[pl.ds(pl.multiple_of(base, 16), tok), :] = kin[p, xs]
        last = kpad[pl.ds(pl.multiple_of(base + tail, 16), 16), :].astype(F32)
        prior = kpad[pl.ds(pl.multiple_of(base + tail - 16, 16), 16), :].astype(F32)
        row = lax.broadcasted_iota(jnp.int32, (16, LANES), 0)
        kpad[pl.ds(pl.multiple_of(base + tail, 16), 16), :] = jnp.where(
            row < tok - tail, last, prior).astype(BF16)
        vaug[pl.ds(pl.multiple_of(base, 16), tok), 0:LANES] = vin[p, xs]
        vaug[pl.ds(pl.multiple_of(base, 16), tok), LANES:2 * LANES] = jnp.ones((tok, LANES), BF16)

    def take(i, carry):
        xs = at_x(i)
        wait(kin.at[c, xs], k_r.at[xs])
        send(kin.at[c, xs], kin.at[c, xs], kf_s.at[xs], kf_r.at[xs], blk=mate)
        wait(vin.at[c, xs], v_r.at[xs])
        send(vin.at[c, xs], vin.at[c, xs], vf_s.at[xs], vf_r.at[xs], blk=mate)
        place(c, xs)
        ticks(i, i + 1)
        return carry

    lax.fori_loop(0, xn, take, 0)

    def take_mate(i, carry):
        xs = at_x(i)
        wait(kin.at[1 - c, xs], kf_r.at[xs])
        wait(vin.at[1 - c, xs], vf_r.at[xs])
        place(1 - c, xs)
        return carry

    lax.fori_loop(0, xn, take_mate, 0)

    lane = lax.broadcasted_iota(jnp.int32, (tok, LANES), 1)
    scale = HD ** -0.5 * LOG2E

    def attend(i, carry):
        xs = at_x(i)
        wait(qin.at[xs], q_r.at[xs])
        qv = qin[xs].astype(F32)
        qpad[0:tok, :] = jnp.where(lane < HD, qv, 0.0).astype(BF16)
        qpad[pitch:pitch + tok, :] = jnp.where(lane < HD, 0.0, qv).astype(BF16)
        scores = lax.dot_general(qpad[...], kpad[...], NT, preferred_element_type=F32)
        top = jnp.max(scores, axis=1, keepdims=True)
        weights = jnp.exp2((scores - top) * scale).astype(BF16)
        mixed = jnp.dot(weights, vaug[...], preferred_element_type=F32)
        both = mixed[:, :LANES] / mixed[:, LANES:]
        ob[xs] = jnp.where(lane < HD, both[0:tok], both[pitch:pitch + tok]).astype(BF16)

        @pl.when(i == 0)
        def _():
            ain[x] = ob[x]

        @pl.when(i > 0)
        def _():
            send(ob.at[xs], ain.at[x], o_s.at[xs], o_r.at[x], blk=2 * xs + c)

        ticks(xn + 2 * i, xn + 2 * i + 2)
        return carry

    lax.fori_loop(0, xn, attend, 0)
    ticks(3 * xn, max(hops) * parts)

    @pl.when(c == 0)
    def _():
        for way in range(2):
            for s in range(hops[way]):
                zz = lax.rem(z + (1 + s if way else 2 * nz - 1 - s), nz)
                for j in range(parts):
                    wait(wall.at[part(j), slab_rows(zz)], p_r.at[way, s, j])

    wait(wall.at[0:9, slab_rows(z)], loc.at[0])
    wait(rbuf, loc.at[1])
    for i in range(1, xn):
        xs = at_x(i)
        wait(ain.at[xs], o_r.at[xs])

    attention = jnp.concatenate([ain[i] for i in range(xn)], axis=1)
    total = rbuf[...].astype(F32)
    convs = taps - (-(-attention.shape[1] // width))
    for b in range(convs, taps):
        lo = (b - convs) * width
        hi = min(lo + width, attention.shape[1])
        total = total + lax.dot_general(
            attention[:, lo:hi], wall[b, :, 0:hi - lo], NT, preferred_element_type=F32)
    hpad[0:tok, :] = total.astype(BF16)

    hid = hpad[...]
    for dc in (1, 0, 2):
        grid[dc, cp:3 * cp, :] = jnp.dot(
            one_hot(2 * cp, pitch, dc, cp, None), hid, preferred_element_type=F32).astype(BF16)
        if dc == 1:
            send(grid.at[1, cp:2 * cp], hin.at[1], h_s.at[0], h_r.at[1],
                 blk=lax.rem(blk + nb - 1, nb))
            send(grid.at[1, 2 * cp:3 * cp], hin.at[0], h_s.at[1], h_r.at[0],
                 blk=lax.rem(blk + 1, nb))

    both_rows = jnp.zeros((2 * cp, out.shape[1]), F32)
    for dc in range(3):
        both_rows += jnp.dot(grid[dc, cp:3 * cp, :], wall[3 + dc], preferred_element_type=F32)
    upper = both_rows[0:cp]
    lower = both_rows[cp:2 * cp]
    for dc in range(3):
        upper += jnp.dot(grid[dc, 2 * cp:3 * cp, :], wall[6 + dc], preferred_element_type=F32)
        lower += jnp.dot(grid[dc, cp:2 * cp, :], wall[dc], preferred_element_type=F32)
    wait(hin.at[0], h_r.at[0])
    wait(hin.at[1], h_r.at[1])
    for dc in range(3):
        above = jnp.dot(one_hot(cp, cp, dc, cp, blk > 0), hin[0], preferred_element_type=F32)
        below = jnp.dot(one_hot(cp, cp, dc, cp, blk < nb - 1), hin[1], preferred_element_type=F32)
        upper += jnp.dot(above.astype(BF16), wall[dc], preferred_element_type=F32)
        lower += jnp.dot(below.astype(BF16), wall[6 + dc], preferred_element_type=F32)
    out[0:cp, :] = upper.astype(BF16)
    out[cp:2 * cp, :] = lower.astype(BF16)

    for i in range(1, xn):
        xs = at_x(i)
        wait(kin.at[c, 0], k_s.at[i])
        wait(vin.at[c, 0], v_s.at[i])
        wait(qin.at[0], q_s.at[i])
        wait(ob.at[xs], o_s.at[xs])
    for i in range(xn):
        wait(kin.at[c, i], kf_s.at[i])
        wait(vin.at[c, i], vf_s.at[i])

    @pl.when(c == 1)
    def _():
        for way in range(2):
            for j in range(parts):
                wait(wall.at[part(j), slab_rows(z)], w_s.at[way, j])
                wait(wall.at[part(j), slab_rows(z)], p_s.at[way, j])

    wait(hin.at[0], h_s.at[0])
    wait(hin.at[1], h_s.at[1])


def body(queries, key_states, value_states, residual, proj_weight, conv_weight):
    nb = lax.axis_size("blk")
    nz = lax.axis_size("batch")
    tok = queries.shape[1]
    slab = conv_weight.shape[2]
    width = conv_weight.shape[3]
    depth = proj_weight.shape[0]
    blocks = -(-depth // width)
    taps = 9 + blocks
    parts = taps // 3
    xn = nb // 2
    pitch = up16(tok)
    cp = up16(COLS)
    feats = nz * slab
    up = (nz - 1) // 3
    hops = (up, nz - 1 - up)
    far = max(hops)
    dma = pltpu.SemaphoreType.DMA
    any_space = pl.BlockSpec(memory_space=pl.ANY)
    got = pl.pallas_call(
        functools.partial(kernel, (nb, nz, tok, slab, taps, pitch, cp, hops)),
        out_shape=jax.ShapeDtypeStruct((2 * cp, width), BF16),
        in_specs=[any_space] * 5 + [pl.BlockSpec(memory_space=pltpu.VMEM)],
        out_specs=pl.BlockSpec(memory_space=pltpu.VMEM),
        scratch_shapes=[
            pltpu.VMEM((2, xn, tok, LANES), BF16),
            pltpu.VMEM((2, xn, tok, LANES), BF16),
            pltpu.VMEM((xn, tok, LANES), BF16),
            pltpu.VMEM((xn, tok, LANES), BF16),
            pltpu.VMEM((xn, tok, LANES), BF16),
            pltpu.VMEM((taps, feats, width), BF16),
            pltpu.VMEM((nb * pitch, LANES), BF16),
            pltpu.VMEM((nb * pitch, 2 * LANES), BF16),
            pltpu.VMEM((2 * pitch, LANES), BF16),
            pltpu.VMEM((pitch, feats), BF16),
            pltpu.VMEM((3, 4 * cp, feats), BF16),
            pltpu.VMEM((2, cp, feats), BF16),
            pltpu.VMEM((tok, feats), BF16),
            dma((xn,)), dma((xn,)), dma((xn,)), dma((xn,)), dma((xn,)), dma((xn,)),
            dma((xn,)), dma((xn,)), dma((xn,)), dma((xn,)), dma((xn,)), dma((xn,)),
            dma((2, parts)), dma((2, far, parts)), dma((2, parts)), dma((2, far, parts)),
            dma((2,)), dma((2,)), dma((2,)), pltpu.SemaphoreType.REGULAR,
            pltpu.VMEM((blocks, slab, width), BF16),
        ],
        compiler_params=pltpu.CompilerParams(
            collective_id=0, has_side_effects=True, vmem_limit_bytes=60 * 1024 * 1024),
    )(queries, key_states, value_states, residual, conv_weight.reshape(9, slab, width), proj_weight)
    return got.reshape(ROWS, cp, width)[:, :COLS].reshape(1, tok, width)


def solution(mesh):
    return jax.shard_map(
        body,
        mesh=mesh,
        in_specs=(
            P(("groups", "batch"), "blk", None),
            P(("groups", "batch"), "blk", None),
            P(("groups", "batch"), "blk", None),
            P(("groups", "batch"), "blk", None),
            P(None, "batch"),
            P(None, None, "batch", None),
        ),
        out_specs=P(("groups", "batch"), "blk", None),
        check_vma=False,
    )
```

```python
import functools

import jax
import jax.numpy as jnp
from jax import lax
from jax.experimental import pallas as pl
from jax.experimental.pallas import tpu as pltpu
from jax.sharding import PartitionSpec as P

HD = 64
COLS = 74
ROWS = 2
LANES = 128
LOG2E = 1.4426950408889634
MESH = pl.DeviceIdType.MESH
F32 = jnp.float32
BF16 = jnp.bfloat16
NT = (((1,), (1,)), ((), ()))


def up16(n):
    return -(-n // 16) * 16


def one_hot(rows, depth, dc, pitch, flag):
    i = lax.broadcasted_iota(jnp.int32, (rows, depth), 0)
    t = lax.broadcasted_iota(jnp.int32, (rows, depth), 1)
    r = jnp.where(i >= pitch, 1, 0)
    c = i - r * pitch
    src = c + (dc - 1)
    ok = (t == r * COLS + src) & (c < COLS) & (src >= 0) & (src < COLS)
    if flag is not None:
        ok = ok & flag
    return jnp.where(ok, 1.0, 0.0).astype(BF16)


def kernel(dims, q, k, v, res, conv, proj, out, kin, vin, qin, ob, ain, wall, kpad, vaug, qpad,
           hpad, grid, hin, rbuf, k_s, k_r, v_s, v_r, q_s, q_r, o_s, o_r, w_s, w_r, p_s, p_r, h_s, h_r, loc, go, flat, even, odd):
    nb, nz, tok, slab, taps, pitch, cp, hops = dims
    xn = nb // 2
    parts = taps // 3
    blk = lax.axis_index("blk")
    z = lax.axis_index("batch")
    x = blk // 2
    c = blk % 2
    mate = 2 * x + 1 - c
    side = lax.rem(blk + nb + 2 * c - 1, nb)
    znext = (lax.rem(z + 1, nz), lax.rem(z + nz - 1, nz))

    def at_x(i):
        off = ((i + 1) // 2) * (2 * (i % 2) - 1)
        return lax.rem(x + off + xn, xn)

    def wait(ref, sem):
        pltpu.make_async_copy(ref, ref, sem).wait()

    def send(src, dst, s_sem, r_sem, **where):
        pltpu.make_async_remote_copy(
            src_ref=src, dst_ref=dst, send_sem=s_sem, recv_sem=r_sem,
            device_id=where, device_id_type=MESH,
        ).start()

    barrier = pltpu.get_barrier_semaphore()
    for i in range(xn):
        d = at_x(i)
        if i > 0:
            pl.semaphore_signal(barrier, inc=1, device_id={"blk": 2 * d}, device_id_type=MESH)
        else:
            @pl.when(c == 1)
            def _():
                pl.semaphore_signal(barrier, inc=1, device_id={"blk": mate}, device_id_type=MESH)

    @pl.when(c == 1)
    def _():
        for n in znext:
            pl.semaphore_signal(barrier, inc=1, device_id={"batch": n}, device_id_type=MESH)

    @pl.when(c == 0)
    def _():
        pl.semaphore_wait(barrier, nb - 1)
        pl.semaphore_signal(go, inc=1, device_id={"blk": mate}, device_id_type=MESH)

    @pl.when(c == 1)
    def _():
        pl.semaphore_wait(go, 1)

    def cols(i):
        return pl.ds(pl.multiple_of(i * LANES, LANES), LANES)

    def slab_rows(zz):
        return pl.ds(pl.multiple_of(zz * slab, slab), slab)

    for i in range(1, xn):
        d = at_x(i)
        send(k.at[0, :, cols(d)], kin.at[c, x], k_s.at[i], k_r.at[c, x], blk=2 * d)
        send(v.at[0, :, cols(d)], vin.at[c, x], v_s.at[i], v_r.at[c, x], blk=2 * d)

    @pl.when(c == 0)
    def _():
        pltpu.make_async_copy(k.at[0, :, cols(x)], kin.at[0, x], k_r.at[0, x]).start()
        pltpu.make_async_copy(v.at[0, :, cols(x)], vin.at[0, x], v_r.at[0, x]).start()
        pltpu.make_async_copy(q.at[0, :, cols(x)], qin.at[0, x], q_r.at[0, x]).start()

    @pl.when(c == 1)
    def _():
        send(k.at[0, :, cols(x)], kin.at[1, x], k_s.at[0], k_r.at[1, x], blk=mate)
        send(v.at[0, :, cols(x)], vin.at[1, x], v_s.at[0], v_r.at[1, x], blk=mate)
        send(q.at[0, :, cols(x)], qin.at[1, x], q_s.at[0], q_r.at[1, x], blk=mate)

    def ask(i):
        d = at_x(i)
        wait(kin.at[0, 0], k_s.at[i])
        wait(vin.at[0, 0], v_s.at[i])
        send(q.at[0, :, cols(d)], qin.at[c, x], q_s.at[i], q_r.at[c, x], blk=2 * d)

    pltpu.make_async_copy(conv, wall.at[0:9, slab_rows(z)], loc.at[0]).start()
    pltpu.make_async_copy(res.at[0], rbuf, loc.at[1]).start()

    def part(j):
        return pl.ds(3 * lax.rem(j + parts - 1, parts), 3)

    width = wall.shape[2]
    depth = proj.shape[0]
    for b in range(taps - 9):
        n = min(width, depth - b * width)
        turned = proj[b * width:b * width + n, :].astype(F32).T.astype(BF16)
        flat[b, :, 0:n] = turned
        if n < width:
            flat[b, :, n:width] = jnp.zeros((slab, width - n), BF16)
        wall[9 + b, slab_rows(z), :] = flat[b]

    @pl.when(c == 1)
    def _():
        pl.semaphore_wait(barrier, 2)
        for j in range(parts):
            first = 3 * ((j + parts - 1) % parts)
            src = flat if first == 9 else conv.at[first:first + 3]
            for way in range(2):
                send(src, wall.at[part(j), slab_rows(z)], w_s.at[way, j], w_r.at[way, 0, j],
                     batch=znext[way])

    lag = 2 * parts

    def tick(t, carry):
        for way in range(2):
            u = t - (0 if hops[way] == max(hops) else lag)
            s = u // parts
            j = u - s * parts
            zz = lax.rem(z + (1 + s if way else 2 * nz - 1 - s), nz)

            @pl.when((u >= 0) & (u < hops[way] * parts))
            def _():
                ref = wall.at[part(j), slab_rows(zz)]
                wait(ref, w_r.at[way, s, j])

                @pl.when(s < hops[way] - 1)
                def _():
                    wait(ref, w_s.at[way, j])
                    send(ref, ref, w_s.at[way, j], w_r.at[way, s + 1, j], batch=znext[way])

                @pl.when(s > 0)
                def _():
                    wait(ref, p_s.at[way, j])

                send(ref, ref, p_s.at[way, j], p_r.at[way, s, j], blk=mate)

        return carry

    kpad[...] = jnp.zeros_like(kpad)
    vaug[...] = jnp.zeros_like(vaug)
    qpad[...] = jnp.zeros_like(qpad)
    hpad[...] = jnp.zeros_like(hpad)

    tail = tok // 16 * 16

    def place(p, xs):
        base = (p * xn + xs) * pitch
        kpad[pl.ds(pl.multiple_of(base, 16), tok), :] = kin[p, xs]
        last = kpad[pl.ds(pl.multiple_of(base + tail, 16), 16), :].astype(F32)
        prior = kpad[pl.ds(pl.multiple_of(base + tail - 16, 16), 16), :].astype(F32)
        row = lax.broadcasted_iota(jnp.int32, (16, LANES), 0)
        kpad[pl.ds(pl.multiple_of(base + tail, 16), 16), :] = jnp.where(
            row < tok - tail, last, prior).astype(BF16)
        vaug[pl.ds(pl.multiple_of(base, 16), tok), 0:LANES] = vin[p, xs]
        vaug[pl.ds(pl.multiple_of(base, 16), tok), LANES:2 * LANES] = jnp.ones((tok, LANES), BF16)

    def take(i, carry):
        xs = at_x(i)
        for p in range(2):
            wait(kin.at[p, xs], k_r.at[p, xs])
            wait(vin.at[p, xs], v_r.at[p, xs])
            place(p, xs)

        @pl.when(i > 0)
        def _():
            ask(i)

        return carry

    lane = lax.broadcasted_iota(jnp.int32, (tok, LANES), 1)
    scale = HD ** -0.5 * LOG2E

    def score(p, xs, held):
        qv = qin[p, xs].astype(F32)
        qpad[p, 0:tok, :] = jnp.where(lane < HD, qv, 0.0).astype(BF16)
        qpad[p, pitch:pitch + tok, :] = jnp.where(lane < HD, 0.0, qv).astype(BF16)
        held[...] = lax.dot_general(qpad[p], kpad[...], NT, preferred_element_type=F32)

    def mix(p, xs, held):
        scores = held[...]
        top = jnp.max(scores, axis=1, keepdims=True)
        weights = jnp.exp2((scores - top) * scale).astype(BF16)
        mixed = jnp.dot(weights, vaug[...], preferred_element_type=F32)
        both = mixed[:, :LANES] / mixed[:, LANES:]
        ob[p, xs] = jnp.where(lane < HD, both[0:tok], both[pitch:pitch + tok]).astype(BF16)

    def attend(i, carry):
        xs = at_x(i)
        after = at_x(jnp.minimum(i + 1, xn - 1))
        wait(qin.at[1, xs], q_r.at[1, xs])
        score(1, xs, odd)
        mix(0, xs, even)

        @pl.when(i == 0)
        def _():
            ain[x] = ob[0, x]

        @pl.when(i > 0)
        def _():
            send(ob.at[0, xs], ain.at[x], o_s.at[0, xs], o_r.at[x], blk=2 * xs)

        @pl.when(i < xn - 1)
        def _():
            wait(qin.at[0, after], q_r.at[0, after])

        score(0, after, even)
        mix(1, xs, odd)
        send(ob.at[1, xs], ain.at[x], o_s.at[1, xs], o_r.at[x], blk=2 * xs + 1)
        return carry

    @pl.when(c == 0)
    def _():
        lax.fori_loop(0, xn, take, 0)
        wait(qin.at[0, x], q_r.at[0, x])
        score(0, x, even)
        lax.fori_loop(0, xn, attend, 0)

    @pl.when(c == 1)
    def _():
        def step(i, carry):
            lax.fori_loop(2 * i - 2, 2 * i, tick, 0)
            ask(i)
            return carry

        lax.fori_loop(1, xn, step, 0)
        last = max(max(hops) * parts, min(hops) * parts + lag)
        lax.fori_loop(2 * xn - 2, last, tick, 0)

    @pl.when(c == 0)
    def _():
        for way in range(2):
            for s in range(hops[way]):
                zz = lax.rem(z + (1 + s if way else 2 * nz - 1 - s), nz)
                for j in range(parts):
                    wait(wall.at[part(j), slab_rows(zz)], p_r.at[way, s, j])

    wait(wall.at[0:9, slab_rows(z)], loc.at[0])
    wait(rbuf, loc.at[1])
    for i in range(1, xn):
        xs = at_x(i)
        wait(ain.at[xs], o_r.at[xs])

    @pl.when(c == 1)
    def _():
        wait(ain.at[x], o_r.at[x])


    attention = jnp.concatenate([ain[i] for i in range(xn)], axis=1)
    total = rbuf[...].astype(F32)
    convs = taps - (-(-attention.shape[1] // width))
    for b in range(convs, taps):
        lo = (b - convs) * width
        hi = min(lo + width, attention.shape[1])
        total = total + lax.dot_general(
            attention[:, lo:hi], wall[b, :, 0:hi - lo], NT, preferred_element_type=F32)
    hpad[0:tok, :] = total.astype(BF16)

    hid = hpad[...]
    for dc in (1, 0, 2):
        grid[dc, cp:3 * cp, :] = jnp.dot(
            one_hot(2 * cp, pitch, dc, cp, None), hid, preferred_element_type=F32).astype(BF16)
        if dc == 1:
            send(grid.at[1, cp:2 * cp], hin.at[1], h_s.at[0], h_r.at[1],
                 blk=lax.rem(blk + nb - 1, nb))
            send(grid.at[1, 2 * cp:3 * cp], hin.at[0], h_s.at[1], h_r.at[0],
                 blk=lax.rem(blk + 1, nb))

    both_rows = jnp.zeros((2 * cp, out.shape[1]), F32)
    for dc in range(3):
        both_rows += jnp.dot(grid[dc, cp:3 * cp, :], wall[3 + dc], preferred_element_type=F32)
    upper = both_rows[0:cp]
    lower = both_rows[cp:2 * cp]
    for dc in range(3):
        upper += jnp.dot(grid[dc, 2 * cp:3 * cp, :], wall[6 + dc], preferred_element_type=F32)
        lower += jnp.dot(grid[dc, cp:2 * cp, :], wall[dc], preferred_element_type=F32)
    wait(hin.at[0], h_r.at[0])
    wait(hin.at[1], h_r.at[1])
    for dc in range(3):
        above = jnp.dot(one_hot(cp, cp, dc, cp, blk > 0), hin[0], preferred_element_type=F32)
        below = jnp.dot(one_hot(cp, cp, dc, cp, blk < nb - 1), hin[1], preferred_element_type=F32)
        upper += jnp.dot(above.astype(BF16), wall[dc], preferred_element_type=F32)
        lower += jnp.dot(below.astype(BF16), wall[6 + dc], preferred_element_type=F32)
    out[0:cp, :] = upper.astype(BF16)
    out[cp:2 * cp, :] = lower.astype(BF16)

    for i in range(1, xn):
        wait(qin.at[0, 0], q_s.at[i])

    @pl.when(c == 0)
    def _():
        for i in range(xn):
            xs = at_x(i)
            if i > 0:
                wait(ob.at[0, xs], o_s.at[0, xs])
            wait(ob.at[1, xs], o_s.at[1, xs])

    @pl.when(c == 1)
    def _():
        wait(kin.at[0, 0], k_s.at[0])
        wait(vin.at[0, 0], v_s.at[0])
        wait(qin.at[0, 0], q_s.at[0])

    @pl.when(c == 1)
    def _():
        for way in range(2):
            for j in range(parts):
                wait(wall.at[part(j), slab_rows(z)], w_s.at[way, j])
                wait(wall.at[part(j), slab_rows(z)], p_s.at[way, j])

    wait(hin.at[0], h_s.at[0])
    wait(hin.at[1], h_s.at[1])


def body(queries, key_states, value_states, residual, proj_weight, conv_weight):
    nb = lax.axis_size("blk")
    nz = lax.axis_size("batch")
    tok = queries.shape[1]
    slab = conv_weight.shape[2]
    width = conv_weight.shape[3]
    depth = proj_weight.shape[0]
    blocks = -(-depth // width)
    taps = 9 + blocks
    parts = taps // 3
    xn = nb // 2
    pitch = up16(tok)
    cp = up16(COLS)
    feats = nz * slab
    up = 2 * (nz - 1) // 5
    hops = (up, nz - 1 - up)
    far = max(hops)
    dma = pltpu.SemaphoreType.DMA
    any_space = pl.BlockSpec(memory_space=pl.ANY)
    got = pl.pallas_call(
        functools.partial(kernel, (nb, nz, tok, slab, taps, pitch, cp, hops)),
        out_shape=jax.ShapeDtypeStruct((2 * cp, width), BF16),
        in_specs=[any_space] * 5 + [pl.BlockSpec(memory_space=pltpu.VMEM)],
        out_specs=pl.BlockSpec(memory_space=pltpu.VMEM),
        scratch_shapes=[
            pltpu.VMEM((2, xn, tok, LANES), BF16),
            pltpu.VMEM((2, xn, tok, LANES), BF16),
            pltpu.VMEM((2, xn, tok, LANES), BF16),
            pltpu.VMEM((2, xn, tok, LANES), BF16),
            pltpu.VMEM((xn, tok, LANES), BF16),
            pltpu.VMEM((taps, feats, width), BF16),
            pltpu.VMEM((nb * pitch, LANES), BF16),
            pltpu.VMEM((nb * pitch, 2 * LANES), BF16),
            pltpu.VMEM((2, 2 * pitch, LANES), BF16),
            pltpu.VMEM((pitch, feats), BF16),
            pltpu.VMEM((3, 4 * cp, feats), BF16),
            pltpu.VMEM((2, cp, feats), BF16),
            pltpu.VMEM((tok, feats), BF16),
            dma((xn,)), dma((2, xn)), dma((xn,)), dma((2, xn)), dma((xn,)), dma((2, xn)),
            dma((2, xn)), dma((xn,)),
            dma((2, parts)), dma((2, far, parts)), dma((2, parts)), dma((2, far, parts)),
            dma((2,)), dma((2,)), dma((2,)), pltpu.SemaphoreType.REGULAR,
            pltpu.VMEM((blocks, slab, width), BF16),
            pltpu.VMEM((2 * pitch, nb * pitch), F32),
            pltpu.VMEM((2 * pitch, nb * pitch), F32),
        ],
        compiler_params=pltpu.CompilerParams(
            collective_id=0, has_side_effects=True, vmem_limit_bytes=60 * 1024 * 1024),
    )(queries, key_states, value_states, residual, conv_weight.reshape(9, slab, width), proj_weight)
    return got.reshape(ROWS, cp, width)[:, :COLS].reshape(1, tok, width)


def solution(mesh):
    return jax.shard_map(
        body,
        mesh=mesh,
        in_specs=(
            P(("groups", "batch"), "blk", None),
            P(("groups", "batch"), "blk", None),
            P(("groups", "batch"), "blk", None),
            P(("groups", "batch"), "blk", None),
            P(None, "batch"),
            P(None, None, "batch", None),
        ),
        out_specs=P(("groups", "batch"), "blk", None),
        check_vma=False,
    )
```

```python
import functools

import jax
import jax.numpy as jnp
from jax import lax
from jax.experimental import pallas as pl
from jax.experimental.pallas import tpu as pltpu
from jax.sharding import PartitionSpec as P

HD = 64
COLS = 74
ROWS = 2
LANES = 128
LOG2E = 1.4426950408889634
MESH = pl.DeviceIdType.MESH
F32 = jnp.float32
BF16 = jnp.bfloat16
NT = (((1,), (1,)), ((), ()))


def up16(n):
    return -(-n // 16) * 16


def one_hot(rows, depth, dc, pitch, flag):
    i = lax.broadcasted_iota(jnp.int32, (rows, depth), 0)
    t = lax.broadcasted_iota(jnp.int32, (rows, depth), 1)
    r = jnp.where(i >= pitch, 1, 0)
    c = i - r * pitch
    src = c + (dc - 1)
    ok = (t == r * COLS + src) & (c < COLS) & (src >= 0) & (src < COLS)
    if flag is not None:
        ok = ok & flag
    return jnp.where(ok, 1.0, 0.0).astype(BF16)


def kernel(dims, q, k, v, res, conv, proj, out, kin, vin, qin, ob, ain, wall, kpad, vaug, qpad,
           hpad, grid, hin, rbuf, k_s, k_r, v_s, v_r, q_s, q_r, o_s, o_r, w_s, w_r, p_s, p_r, h_s, h_r, loc, go, flat, even, odd, y_s, y_r):
    nb, nz, tok, slab, taps, pitch, cp, hops = dims
    xn = nb // 2
    parts = taps // 3
    blk = lax.axis_index("blk")
    z = lax.axis_index("batch")
    g = lax.axis_index("groups")
    other = g + 1 - 2 * (g % 2)
    x = blk // 2
    c = blk % 2
    mate = 2 * x + 1 - c
    side = lax.rem(blk + nb + 2 * c - 1, nb)
    znext = (lax.rem(z + 1, nz), lax.rem(z + nz - 1, nz))

    def at_x(i):
        off = ((i + 1) // 2) * (2 * (i % 2) - 1)
        return lax.rem(x + off + xn, xn)

    def wait(ref, sem):
        pltpu.make_async_copy(ref, ref, sem).wait()

    def send(src, dst, s_sem, r_sem, **where):
        pltpu.make_async_remote_copy(
            src_ref=src, dst_ref=dst, send_sem=s_sem, recv_sem=r_sem,
            device_id=where, device_id_type=MESH,
        ).start()

    barrier = pltpu.get_barrier_semaphore()
    for i in range(xn):
        d = at_x(i)
        if i > 0:
            pl.semaphore_signal(barrier, inc=1, device_id={"blk": 2 * d}, device_id_type=MESH)
        else:
            @pl.when(c == 1)
            def _():
                pl.semaphore_signal(barrier, inc=1, device_id={"blk": mate}, device_id_type=MESH)

    @pl.when(c == 1)
    def _():
        for n in znext:
            pl.semaphore_signal(barrier, inc=1, device_id={"batch": n}, device_id_type=MESH)
        pl.semaphore_signal(barrier, inc=1, device_id={"groups": other}, device_id_type=MESH)

    @pl.when(c == 0)
    def _():
        pl.semaphore_wait(barrier, nb - 1)
        pl.semaphore_signal(go, inc=1, device_id={"blk": mate}, device_id_type=MESH)

    @pl.when(c == 1)
    def _():
        pl.semaphore_wait(go, 1)

    def cols(i):
        return pl.ds(pl.multiple_of(i * LANES, LANES), LANES)

    def slab_rows(zz):
        return pl.ds(pl.multiple_of(zz * slab, slab), slab)

    for i in range(1, xn):
        d = at_x(i)
        send(k.at[0, :, cols(d)], kin.at[c, x], k_s.at[i], k_r.at[c, x], blk=2 * d)
        send(v.at[0, :, cols(d)], vin.at[c, x], v_s.at[i], v_r.at[c, x], blk=2 * d)

    @pl.when(c == 0)
    def _():
        pltpu.make_async_copy(k.at[0, :, cols(x)], kin.at[0, x], k_r.at[0, x]).start()
        pltpu.make_async_copy(v.at[0, :, cols(x)], vin.at[0, x], v_r.at[0, x]).start()
        pltpu.make_async_copy(q.at[0, :, cols(x)], qin.at[0, x], q_r.at[0, x]).start()

    @pl.when(c == 1)
    def _():
        send(k.at[0, :, cols(x)], kin.at[1, x], k_s.at[0], k_r.at[1, x], blk=mate)
        send(v.at[0, :, cols(x)], vin.at[1, x], v_s.at[0], v_r.at[1, x], blk=mate)
        send(q.at[0, :, cols(x)], qin.at[1, x], q_s.at[0], q_r.at[1, x], blk=mate)

    def ask(i):
        d = at_x(i)
        wait(kin.at[0, 0], k_s.at[i])
        wait(vin.at[0, 0], v_s.at[i])
        send(q.at[0, :, cols(d)], qin.at[c, x], q_s.at[i], q_r.at[c, x], blk=2 * d)

    pltpu.make_async_copy(conv, wall.at[0:9, slab_rows(z)], loc.at[0]).start()
    pltpu.make_async_copy(res.at[0], rbuf, loc.at[1]).start()

    def part(j):
        mine, theirs = 3 + 3 * (g % 2), 6 - 3 * (g % 2)
        if isinstance(j, int):
            return pl.ds((9, 0, mine, theirs)[j], 3)
        return pl.ds(jnp.where(j == 0, 9, jnp.where(j == 1, 0, jnp.where(j == 2, mine, theirs))), 3)

    width = wall.shape[2]
    depth = proj.shape[0]
    for b in range(taps - 9):
        n = min(width, depth - b * width)
        turned = proj[b * width:b * width + n, :].astype(F32).T.astype(BF16)
        flat[b, :, 0:n] = turned
        if n < width:
            flat[b, :, n:width] = jnp.zeros((slab, width - n), BF16)
        wall[9 + b, slab_rows(z), :] = flat[b]

    @pl.when(c == 1)
    def _():
        pl.semaphore_wait(barrier, 3)
        for j in range(parts - 1):
            src = flat if j == 0 else conv.at[part(j)]
            for way in range(2):
                send(src, wall.at[part(j), slab_rows(z)], w_s.at[way, j], w_r.at[way, 0, j],
                     batch=znext[way])

    lag = 2 * parts

    def hand(way, s):
        zz = lax.rem(z + (1 + s if way else 2 * nz - 1 - s), nz)
        ref = wall.at[part(parts - 1), slab_rows(zz)]
        wait(ref, y_r.at[way, s])

        @pl.when(s > 0)
        def _():
            wait(ref, p_s.at[way, parts - 1])

        send(ref, ref, p_s.at[way, parts - 1], p_r.at[way, s, parts - 1], blk=mate)

    def tick(t, carry):
        for way in range(2):
            u = t - (0 if hops[way] == max(hops) else lag)
            s = u // parts
            j = u - s * parts
            zz = lax.rem(z + (1 + s if way else 2 * nz - 1 - s), nz)

            inside = (u >= 0) & (u < hops[way] * parts)

            @pl.when(inside & (j < parts - 1))
            def _():
                ref = wall.at[part(j), slab_rows(zz)]
                wait(ref, w_r.at[way, s, j])

                @pl.when(s < hops[way] - 1)
                def _():
                    wait(ref, w_s.at[way, j])
                    send(ref, ref, w_s.at[way, j], w_r.at[way, s + 1, j], batch=znext[way])

                @pl.when(j == parts - 2)
                def _():
                    @pl.when(s > 0)
                    def _():
                        wait(ref, y_s.at[way])

                    send(ref, ref, y_s.at[way], y_r.at[way, s], groups=other)

                @pl.when(s > 0)
                def _():
                    wait(ref, p_s.at[way, j])

                send(ref, ref, p_s.at[way, j], p_r.at[way, s, j], blk=mate)

            @pl.when(inside & (j == parts - 1) & (s > 0))
            def _():
                hand(way, s - 1)

        return carry

    kpad[...] = jnp.zeros_like(kpad)
    vaug[...] = jnp.zeros_like(vaug)
    qpad[...] = jnp.zeros_like(qpad)
    hpad[...] = jnp.zeros_like(hpad)

    tail = tok // 16 * 16

    def place(p, xs):
        base = (p * xn + xs) * pitch
        kpad[pl.ds(pl.multiple_of(base, 16), tok), :] = kin[p, xs]
        last = kpad[pl.ds(pl.multiple_of(base + tail, 16), 16), :].astype(F32)
        prior = kpad[pl.ds(pl.multiple_of(base + tail - 16, 16), 16), :].astype(F32)
        row = lax.broadcasted_iota(jnp.int32, (16, LANES), 0)
        kpad[pl.ds(pl.multiple_of(base + tail, 16), 16), :] = jnp.where(
            row < tok - tail, last, prior).astype(BF16)
        vaug[pl.ds(pl.multiple_of(base, 16), tok), 0:LANES] = vin[p, xs]
        vaug[pl.ds(pl.multiple_of(base, 16), tok), LANES:2 * LANES] = jnp.ones((tok, LANES), BF16)

    def take(i, carry):
        xs = at_x(i)
        for p in range(2):
            wait(kin.at[p, xs], k_r.at[p, xs])
            wait(vin.at[p, xs], v_r.at[p, xs])
            place(p, xs)

        @pl.when(i > 0)
        def _():
            ask(i)

        return carry

    lane = lax.broadcasted_iota(jnp.int32, (tok, LANES), 1)
    scale = HD ** -0.5 * LOG2E

    keys = kpad.shape[0]
    piece = keys // 5

    def spread(p, xs):
        qv = qin[p, xs].astype(F32)
        qpad[p, 0:tok, :] = jnp.where(lane < HD, qv, 0.0).astype(BF16)
        qpad[p, pitch:pitch + tok, :] = jnp.where(lane < HD, 0.0, qv).astype(BF16)

    def score(p, held, lo):
        held[:, lo:lo + piece] = lax.dot_general(
            qpad[p], kpad[lo:lo + piece, :], NT, preferred_element_type=F32)

    def work(p, xs, held, p_next, xs_next, held_next):
        spread(p_next, xs_next)
        top = jnp.max(held[...], axis=1, keepdims=True)
        mixed = jnp.zeros((2 * pitch, 2 * LANES), F32)
        for lo in range(0, keys, piece):
            score(p_next, held_next, lo)
            weights = jnp.exp2((held[:, lo:lo + piece] - top) * scale).astype(BF16)
            mixed += jnp.dot(weights, vaug[lo:lo + piece, :], preferred_element_type=F32)
        both = mixed[:, :LANES] / mixed[:, LANES:]
        ob[p, xs] = jnp.where(lane < HD, both[0:tok], both[pitch:pitch + tok]).astype(BF16)

    def attend(i, carry):
        xs = at_x(i)
        after = at_x(jnp.minimum(i + 1, xn - 1))
        wait(qin.at[1, xs], q_r.at[1, xs])
        work(0, xs, even, 1, xs, odd)

        @pl.when(i == 0)
        def _():
            ain[x] = ob[0, x]

        @pl.when(i > 0)
        def _():
            send(ob.at[0, xs], ain.at[x], o_s.at[0, xs], o_r.at[x], blk=2 * xs)

        @pl.when(i < xn - 1)
        def _():
            wait(qin.at[0, after], q_r.at[0, after])

        work(1, xs, odd, 0, after, even)
        send(ob.at[1, xs], ain.at[x], o_s.at[1, xs], o_r.at[x], blk=2 * xs + 1)
        return carry

    @pl.when(c == 0)
    def _():
        lax.fori_loop(0, xn, take, 0)
        wait(qin.at[0, x], q_r.at[0, x])
        spread(0, x)
        for lo in range(0, keys, piece):
            score(0, even, lo)
        lax.fori_loop(0, xn, attend, 0)

    @pl.when(c == 1)
    def _():
        def step(i, carry):
            lax.fori_loop(2 * i - 2, 2 * i, tick, 0)
            ask(i)
            return carry

        lax.fori_loop(1, xn, step, 0)
        last = max(max(hops) * parts, min(hops) * parts + lag)
        lax.fori_loop(2 * xn - 2, last, tick, 0)
        for way in range(2):
            hand(way, jnp.int32(hops[way] - 1))

    @pl.when(c == 0)
    def _():
        for way in range(2):
            for s in range(hops[way]):
                zz = lax.rem(z + (1 + s if way else 2 * nz - 1 - s), nz)
                for j in range(parts):
                    wait(wall.at[part(j), slab_rows(zz)], p_r.at[way, s, j])

    wait(wall.at[0:9, slab_rows(z)], loc.at[0])
    wait(rbuf, loc.at[1])
    for i in range(1, xn):
        xs = at_x(i)
        wait(ain.at[xs], o_r.at[xs])

    @pl.when(c == 1)
    def _():
        wait(ain.at[x], o_r.at[x])


    attention = jnp.concatenate([ain[i] for i in range(xn)], axis=1)
    total = rbuf[...].astype(F32)
    convs = taps - (-(-attention.shape[1] // width))
    for b in range(convs, taps):
        lo = (b - convs) * width
        hi = min(lo + width, attention.shape[1])
        total = total + lax.dot_general(
            attention[:, lo:hi], wall[b, :, 0:hi - lo], NT, preferred_element_type=F32)
    hpad[0:tok, :] = total.astype(BF16)

    hid = hpad[...]
    for dc in (1, 0, 2):
        grid[dc, cp:3 * cp, :] = jnp.dot(
            one_hot(2 * cp, pitch, dc, cp, None), hid, preferred_element_type=F32).astype(BF16)
        if dc == 1:
            send(grid.at[1, cp:2 * cp], hin.at[1], h_s.at[0], h_r.at[1],
                 blk=lax.rem(blk + nb - 1, nb))
            send(grid.at[1, 2 * cp:3 * cp], hin.at[0], h_s.at[1], h_r.at[0],
                 blk=lax.rem(blk + 1, nb))

    both_rows = jnp.zeros((2 * cp, out.shape[1]), F32)
    for dc in range(3):
        both_rows += jnp.dot(grid[dc, cp:3 * cp, :], wall[3 + dc], preferred_element_type=F32)
    upper = both_rows[0:cp]
    lower = both_rows[cp:2 * cp]
    for dc in range(3):
        upper += jnp.dot(grid[dc, 2 * cp:3 * cp, :], wall[6 + dc], preferred_element_type=F32)
        lower += jnp.dot(grid[dc, cp:2 * cp, :], wall[dc], preferred_element_type=F32)
    wait(hin.at[0], h_r.at[0])
    wait(hin.at[1], h_r.at[1])
    for dc in range(3):
        above = jnp.dot(one_hot(cp, cp, dc, cp, blk > 0), hin[0], preferred_element_type=F32)
        below = jnp.dot(one_hot(cp, cp, dc, cp, blk < nb - 1), hin[1], preferred_element_type=F32)
        upper += jnp.dot(above.astype(BF16), wall[dc], preferred_element_type=F32)
        lower += jnp.dot(below.astype(BF16), wall[6 + dc], preferred_element_type=F32)
    out[0:cp, :] = upper.astype(BF16)
    out[cp:2 * cp, :] = lower.astype(BF16)

    for i in range(1, xn):
        wait(qin.at[0, 0], q_s.at[i])

    @pl.when(c == 0)
    def _():
        for i in range(xn):
            xs = at_x(i)
            if i > 0:
                wait(ob.at[0, xs], o_s.at[0, xs])
            wait(ob.at[1, xs], o_s.at[1, xs])

    @pl.when(c == 1)
    def _():
        wait(kin.at[0, 0], k_s.at[0])
        wait(vin.at[0, 0], v_s.at[0])
        wait(qin.at[0, 0], q_s.at[0])

    @pl.when(c == 1)
    def _():
        for way in range(2):
            wait(wall.at[part(0), slab_rows(z)], y_s.at[way])
            for j in range(parts):
                if j < parts - 1:
                    wait(wall.at[part(j), slab_rows(z)], w_s.at[way, j])
                wait(wall.at[part(j), slab_rows(z)], p_s.at[way, j])

    wait(hin.at[0], h_s.at[0])
    wait(hin.at[1], h_s.at[1])


def body(queries, key_states, value_states, residual, proj_weight, conv_weight):
    nb = lax.axis_size("blk")
    nz = lax.axis_size("batch")
    tok = queries.shape[1]
    slab = conv_weight.shape[2]
    width = conv_weight.shape[3]
    depth = proj_weight.shape[0]
    blocks = -(-depth // width)
    taps = 9 + blocks
    parts = taps // 3
    xn = nb // 2
    pitch = up16(tok)
    cp = up16(COLS)
    feats = nz * slab
    up = 2 * (nz - 1) // 5
    hops = (up, nz - 1 - up)
    far = max(hops)
    dma = pltpu.SemaphoreType.DMA
    any_space = pl.BlockSpec(memory_space=pl.ANY)
    got = pl.pallas_call(
        functools.partial(kernel, (nb, nz, tok, slab, taps, pitch, cp, hops)),
        out_shape=jax.ShapeDtypeStruct((2 * cp, width), BF16),
        in_specs=[any_space] * 5 + [pl.BlockSpec(memory_space=pltpu.VMEM)],
        out_specs=pl.BlockSpec(memory_space=pltpu.VMEM),
        scratch_shapes=[
            pltpu.VMEM((2, xn, tok, LANES), BF16),
            pltpu.VMEM((2, xn, tok, LANES), BF16),
            pltpu.VMEM((2, xn, tok, LANES), BF16),
            pltpu.VMEM((2, xn, tok, LANES), BF16),
            pltpu.VMEM((xn, tok, LANES), BF16),
            pltpu.VMEM((taps, feats, width), BF16),
            pltpu.VMEM((nb * pitch, LANES), BF16),
            pltpu.VMEM((nb * pitch, 2 * LANES), BF16),
            pltpu.VMEM((2, 2 * pitch, LANES), BF16),
            pltpu.VMEM((pitch, feats), BF16),
            pltpu.VMEM((3, 4 * cp, feats), BF16),
            pltpu.VMEM((2, cp, feats), BF16),
            pltpu.VMEM((tok, feats), BF16),
            dma((xn,)), dma((2, xn)), dma((xn,)), dma((2, xn)), dma((xn,)), dma((2, xn)),
            dma((2, xn)), dma((xn,)),
            dma((2, parts)), dma((2, far, parts)), dma((2, parts)), dma((2, far, parts)),
            dma((2,)), dma((2,)), dma((2,)), pltpu.SemaphoreType.REGULAR,
            pltpu.VMEM((blocks, slab, width), BF16),
            pltpu.VMEM((2 * pitch, nb * pitch), F32),
            pltpu.VMEM((2 * pitch, nb * pitch), F32),
            dma((2,)), dma((2, far)),
        ],
        compiler_params=pltpu.CompilerParams(
            collective_id=0, has_side_effects=True, vmem_limit_bytes=60 * 1024 * 1024),
    )(queries, key_states, value_states, residual, conv_weight.reshape(9, slab, width), proj_weight)
    return got.reshape(ROWS, cp, width)[:, :COLS].reshape(1, tok, width)


def solution(mesh):
    return jax.shard_map(
        body,
        mesh=mesh,
        in_specs=(
            P(("groups", "batch"), "blk", None),
            P(("groups", "batch"), "blk", None),
            P(("groups", "batch"), "blk", None),
            P(("groups", "batch"), "blk", None),
            P(None, "batch"),
            P(None, None, "batch", None),
        ),
        out_specs=P(("groups", "batch"), "blk", None),
        check_vma=False,
    )
```

```python
import functools

import jax
import jax.numpy as jnp
from jax import lax
from jax.experimental import pallas as pl
from jax.experimental.pallas import tpu as pltpu
from jax.sharding import PartitionSpec as P

HD = 64
COLS = 74
ROWS = 2
LANES = 128
LOG2E = 1.4426950408889634
MESH = pl.DeviceIdType.MESH
F32 = jnp.float32
BF16 = jnp.bfloat16
NT = (((1,), (1,)), ((), ()))


def up16(n):
    return -(-n // 16) * 16


def one_hot(rows, depth, dc, pitch, flag):
    i = lax.broadcasted_iota(jnp.int32, (rows, depth), 0)
    t = lax.broadcasted_iota(jnp.int32, (rows, depth), 1)
    r = jnp.where(i >= pitch, 1, 0)
    c = i - r * pitch
    src = c + (dc - 1)
    ok = (t == r * COLS + src) & (c < COLS) & (src >= 0) & (src < COLS)
    if flag is not None:
        ok = ok & flag
    return jnp.where(ok, 1.0, 0.0).astype(BF16)


def kernel(dims, q, k, v, res, conv, proj, out, kin, vin, qin, ob, ain, wall, kpad, vaug, qpad,
           hpad, grid, hin, rbuf, k_s, k_r, v_s, v_r, q_s, q_r, o_s, o_r, w_s, w_r, p_s, p_r, h_s, h_r, loc, go, flat, even, odd, y_s, y_r):
    nb, nz, tok, slab, taps, pitch, cp, hops = dims
    xn = nb // 2
    parts = taps // 3
    blk = lax.axis_index("blk")
    z = lax.axis_index("batch")
    g = lax.axis_index("groups")
    other = g + 1 - 2 * (g % 2)
    x = blk // 2
    c = blk % 2
    mate = 2 * x + 1 - c
    side = lax.rem(blk + nb + 2 * c - 1, nb)
    znext = (lax.rem(z + 1, nz), lax.rem(z + nz - 1, nz))

    def at_x(i):
        off = ((i + 1) // 2) * (2 * (i % 2) - 1)
        return lax.rem(x + off + xn, xn)

    def wait(ref, sem):
        pltpu.make_async_copy(ref, ref, sem).wait()

    def send(src, dst, s_sem, r_sem, **where):
        pltpu.make_async_remote_copy(
            src_ref=src, dst_ref=dst, send_sem=s_sem, recv_sem=r_sem,
            device_id=where, device_id_type=MESH,
        ).start()

    barrier = pltpu.get_barrier_semaphore()
    for i in range(xn):
        d = at_x(i)
        if i > 0:
            pl.semaphore_signal(barrier, inc=1, device_id={"blk": 2 * d}, device_id_type=MESH)
        else:
            @pl.when(c == 1)
            def _():
                pl.semaphore_signal(barrier, inc=1, device_id={"blk": mate}, device_id_type=MESH)

    @pl.when(c == 1)
    def _():
        for n in znext:
            pl.semaphore_signal(barrier, inc=1, device_id={"batch": n}, device_id_type=MESH)
        pl.semaphore_signal(barrier, inc=1, device_id={"groups": other}, device_id_type=MESH)

    @pl.when(c == 0)
    def _():
        pl.semaphore_wait(barrier, nb - 1)
        pl.semaphore_signal(go, inc=1, device_id={"blk": mate}, device_id_type=MESH)

    @pl.when(c == 1)
    def _():
        pl.semaphore_wait(go, 1)

    def cols(i):
        return pl.ds(pl.multiple_of(i * LANES, LANES), LANES)

    def slab_rows(zz):
        return pl.ds(pl.multiple_of(zz * slab, slab), slab)

    for i in range(1, xn):
        d = at_x(i)
        send(k.at[0, :, cols(d)], kin.at[c, x], k_s.at[i], k_r.at[c, x], blk=2 * d)
        send(v.at[0, :, cols(d)], vin.at[c, x], v_s.at[i], v_r.at[c, x], blk=2 * d)

    @pl.when(c == 0)
    def _():
        pltpu.make_async_copy(k.at[0, :, cols(x)], kin.at[0, x], k_r.at[0, x]).start()
        pltpu.make_async_copy(v.at[0, :, cols(x)], vin.at[0, x], v_r.at[0, x]).start()
        pltpu.make_async_copy(q.at[0, :, cols(x)], qin.at[0, x], q_r.at[0, x]).start()

    @pl.when(c == 1)
    def _():
        send(k.at[0, :, cols(x)], kin.at[1, x], k_s.at[0], k_r.at[1, x], blk=mate)
        send(v.at[0, :, cols(x)], vin.at[1, x], v_s.at[0], v_r.at[1, x], blk=mate)
        send(q.at[0, :, cols(x)], qin.at[1, x], q_s.at[0], q_r.at[1, x], blk=mate)

    def ask(i):
        d = at_x(i)
        wait(kin.at[0, 0], k_s.at[i])
        wait(vin.at[0, 0], v_s.at[i])
        send(q.at[0, :, cols(d)], qin.at[c, x], q_s.at[i], q_r.at[c, x], blk=2 * d)

    pltpu.make_async_copy(conv, wall.at[0:9, slab_rows(z)], loc.at[0]).start()
    pltpu.make_async_copy(res.at[0], rbuf, loc.at[1]).start()

    def part(j):
        mine, theirs = 3 + 3 * (g % 2), 6 - 3 * (g % 2)
        if isinstance(j, int):
            return pl.ds((9, 0, mine, theirs)[j], 3)
        return pl.ds(jnp.where(j == 0, 9, jnp.where(j == 1, 0, jnp.where(j == 2, mine, theirs))), 3)

    width = wall.shape[2]
    depth = proj.shape[0]
    for b in range(taps - 9):
        n = min(width, depth - b * width)
        turned = proj[b * width:b * width + n, :].astype(F32).T.astype(BF16)
        flat[b, :, 0:n] = turned
        if n < width:
            flat[b, :, n:width] = jnp.zeros((slab, width - n), BF16)
        wall[9 + b, slab_rows(z), :] = flat[b]

    @pl.when(c == 1)
    def _():
        pl.semaphore_wait(barrier, 3)
        for j in range(parts - 1):
            src = flat if j == 0 else conv.at[part(j)]
            for way in range(2):
                send(src, wall.at[part(j), slab_rows(z)], w_s.at[way, j], w_r.at[way, 0, j],
                     batch=znext[way])

    lag = 2 * parts

    def hand(way, s):
        zz = lax.rem(z + (1 + s if way else 2 * nz - 1 - s), nz)
        ref = wall.at[part(parts - 1), slab_rows(zz)]
        wait(ref, y_r.at[way, s])

        @pl.when(s > 0)
        def _():
            wait(ref, p_s.at[way, parts - 1])

        send(ref, ref, p_s.at[way, parts - 1], p_r.at[way, s, parts - 1], blk=mate)

    def tick(t, carry):
        for way in range(2):
            u = t - (0 if hops[way] == max(hops) else lag)
            s = u // parts
            j = u - s * parts
            zz = lax.rem(z + (1 + s if way else 2 * nz - 1 - s), nz)

            inside = (u >= 0) & (u < hops[way] * parts)

            @pl.when(inside & (j < parts - 1))
            def _():
                ref = wall.at[part(j), slab_rows(zz)]
                wait(ref, w_r.at[way, s, j])

                @pl.when(s < hops[way] - 1)
                def _():
                    wait(ref, w_s.at[way, j])
                    send(ref, ref, w_s.at[way, j], w_r.at[way, s + 1, j], batch=znext[way])

                @pl.when(j == parts - 2)
                def _():
                    @pl.when(s > 0)
                    def _():
                        wait(ref, y_s.at[way])

                    send(ref, ref, y_s.at[way], y_r.at[way, s], groups=other)

                @pl.when(s > 0)
                def _():
                    wait(ref, p_s.at[way, j])

                send(ref, ref, p_s.at[way, j], p_r.at[way, s, j], blk=mate)

            @pl.when(inside & (j == parts - 1) & (s > 0))
            def _():
                hand(way, s - 1)

        return carry

    kpad[...] = jnp.zeros_like(kpad)
    vaug[...] = jnp.zeros_like(vaug)
    qpad[...] = jnp.zeros_like(qpad)
    hpad[...] = jnp.zeros_like(hpad)

    tail = tok // 16 * 16

    def place(p, xs):
        base = (p * xn + xs) * pitch
        kpad[pl.ds(pl.multiple_of(base, 16), tok), :] = kin[p, xs]
        last = kpad[pl.ds(pl.multiple_of(base + tail, 16), 16), :].astype(F32)
        prior = kpad[pl.ds(pl.multiple_of(base + tail - 16, 16), 16), :].astype(F32)
        row = lax.broadcasted_iota(jnp.int32, (16, LANES), 0)
        kpad[pl.ds(pl.multiple_of(base + tail, 16), 16), :] = jnp.where(
            row < tok - tail, last, prior).astype(BF16)
        vaug[pl.ds(pl.multiple_of(base, 16), tok), 0:LANES] = vin[p, xs]
        vaug[pl.ds(pl.multiple_of(base, 16), tok), LANES:2 * LANES] = jnp.ones((tok, LANES), BF16)

    def take(i, carry):
        xs = at_x(i)
        for p in range(2):
            wait(kin.at[p, xs], k_r.at[p, xs])
            wait(vin.at[p, xs], v_r.at[p, xs])
            place(p, xs)

        @pl.when(i > 0)
        def _():
            ask(i)

        return carry

    lane = lax.broadcasted_iota(jnp.int32, (tok, LANES), 1)
    scale = HD ** -0.5 * LOG2E

    keys = kpad.shape[0]
    piece = keys // 5

    def spread(p, xs):
        qv = qin[p, xs].astype(F32)
        qpad[p, 0:tok, :] = jnp.where(lane < HD, qv, 0.0).astype(BF16)
        qpad[p, pitch:pitch + tok, :] = jnp.where(lane < HD, 0.0, qv).astype(BF16)

    def score(p, held, lo):
        held[:, lo:lo + piece] = lax.dot_general(
            qpad[p], kpad[lo:lo + piece, :], NT, preferred_element_type=F32)

    def work(p, xs, held, p_next, xs_next, held_next):
        spread(p_next, xs_next)
        top = jnp.max(held[...], axis=1, keepdims=True)
        mixed = jnp.zeros((2 * pitch, 2 * LANES), F32)
        for lo in range(0, keys, piece):
            score(p_next, held_next, lo)
            weights = jnp.exp2((held[:, lo:lo + piece] - top) * scale).astype(BF16)
            mixed += jnp.dot(weights, vaug[lo:lo + piece, :], preferred_element_type=F32)
        both = mixed[:, :LANES] / mixed[:, LANES:]
        ob[p, xs] = jnp.where(lane < HD, both[0:tok], both[pitch:pitch + tok]).astype(BF16)

    def attend(i, carry):
        xs = at_x(i)
        after = at_x(jnp.minimum(i + 1, xn - 1))
        wait(qin.at[1, xs], q_r.at[1, xs])
        work(0, xs, even, 1, xs, odd)

        @pl.when(i == 0)
        def _():
            ain[x] = ob[0, x]

        @pl.when(i > 0)
        def _():
            send(ob.at[0, xs], ain.at[x], o_s.at[0, xs], o_r.at[x], blk=2 * xs)

        @pl.when(i < xn - 1)
        def _():
            wait(qin.at[0, after], q_r.at[0, after])

        work(1, xs, odd, 0, after, even)
        send(ob.at[1, xs], ain.at[x], o_s.at[1, xs], o_r.at[x], blk=2 * xs + 1)
        return carry

    @pl.when(c == 0)
    def _():
        lax.fori_loop(0, xn, take, 0)
        wait(qin.at[0, x], q_r.at[0, x])
        spread(0, x)
        for lo in range(0, keys, piece):
            score(0, even, lo)
        lax.fori_loop(0, xn, attend, 0)

    @pl.when(c == 1)
    def _():
        def step(i, carry):
            lax.fori_loop(3 * i - 3, 3 * i, tick, 0)
            ask(i)
            return carry

        lax.fori_loop(1, xn, step, 0)
        last = max(max(hops) * parts, min(hops) * parts + lag)
        lax.fori_loop(3 * xn - 3, last, tick, 0)
        for way in range(2):
            hand(way, jnp.int32(hops[way] - 1))

    @pl.when(c == 0)
    def _():
        for way in range(2):
            for s in range(hops[way]):
                zz = lax.rem(z + (1 + s if way else 2 * nz - 1 - s), nz)
                for j in range(parts):
                    wait(wall.at[part(j), slab_rows(zz)], p_r.at[way, s, j])

    wait(wall.at[0:9, slab_rows(z)], loc.at[0])
    wait(rbuf, loc.at[1])
    for i in range(1, xn):
        xs = at_x(i)
        wait(ain.at[xs], o_r.at[xs])

    @pl.when(c == 1)
    def _():
        wait(ain.at[x], o_r.at[x])


    attention = jnp.concatenate([ain[i] for i in range(xn)], axis=1)
    total = rbuf[...].astype(F32)
    convs = taps - (-(-attention.shape[1] // width))
    for b in range(convs, taps):
        lo = (b - convs) * width
        hi = min(lo + width, attention.shape[1])
        total = total + lax.dot_general(
            attention[:, lo:hi], wall[b, :, 0:hi - lo], NT, preferred_element_type=F32)
    hpad[0:tok, :] = total.astype(BF16)

    hid = hpad[...]
    for dc in (1, 0, 2):
        grid[dc, cp:3 * cp, :] = jnp.dot(
            one_hot(2 * cp, pitch, dc, cp, None), hid, preferred_element_type=F32).astype(BF16)
        if dc == 1:
            send(grid.at[1, cp:2 * cp], hin.at[1], h_s.at[0], h_r.at[1],
                 blk=lax.rem(blk + nb - 1, nb))
            send(grid.at[1, 2 * cp:3 * cp], hin.at[0], h_s.at[1], h_r.at[0],
                 blk=lax.rem(blk + 1, nb))

    both_rows = jnp.zeros((2 * cp, out.shape[1]), F32)
    for dc in range(3):
        both_rows += jnp.dot(grid[dc, cp:3 * cp, :], wall[3 + dc], preferred_element_type=F32)
    upper = both_rows[0:cp]
    lower = both_rows[cp:2 * cp]
    for dc in range(3):
        upper += jnp.dot(grid[dc, 2 * cp:3 * cp, :], wall[6 + dc], preferred_element_type=F32)
        lower += jnp.dot(grid[dc, cp:2 * cp, :], wall[dc], preferred_element_type=F32)
    wait(hin.at[0], h_r.at[0])
    wait(hin.at[1], h_r.at[1])
    for dc in range(3):
        above = jnp.dot(one_hot(cp, cp, dc, cp, blk > 0), hin[0], preferred_element_type=F32)
        below = jnp.dot(one_hot(cp, cp, dc, cp, blk < nb - 1), hin[1], preferred_element_type=F32)
        upper += jnp.dot(above.astype(BF16), wall[dc], preferred_element_type=F32)
        lower += jnp.dot(below.astype(BF16), wall[6 + dc], preferred_element_type=F32)
    out[0:cp, :] = upper.astype(BF16)
    out[cp:2 * cp, :] = lower.astype(BF16)

    for i in range(1, xn):
        wait(qin.at[0, 0], q_s.at[i])

    @pl.when(c == 0)
    def _():
        for i in range(xn):
            xs = at_x(i)
            if i > 0:
                wait(ob.at[0, xs], o_s.at[0, xs])
            wait(ob.at[1, xs], o_s.at[1, xs])

    @pl.when(c == 1)
    def _():
        wait(kin.at[0, 0], k_s.at[0])
        wait(vin.at[0, 0], v_s.at[0])
        wait(qin.at[0, 0], q_s.at[0])

    @pl.when(c == 1)
    def _():
        for way in range(2):
            wait(wall.at[part(0), slab_rows(z)], y_s.at[way])
            for j in range(parts):
                if j < parts - 1:
                    wait(wall.at[part(j), slab_rows(z)], w_s.at[way, j])
                wait(wall.at[part(j), slab_rows(z)], p_s.at[way, j])

    wait(hin.at[0], h_s.at[0])
    wait(hin.at[1], h_s.at[1])


def body(queries, key_states, value_states, residual, proj_weight, conv_weight):
    nb = lax.axis_size("blk")
    nz = lax.axis_size("batch")
    tok = queries.shape[1]
    slab = conv_weight.shape[2]
    width = conv_weight.shape[3]
    depth = proj_weight.shape[0]
    blocks = -(-depth // width)
    taps = 9 + blocks
    parts = taps // 3
    xn = nb // 2
    pitch = up16(tok)
    cp = up16(COLS)
    feats = nz * slab
    up = 2 * (nz - 1) // 5
    hops = (up, nz - 1 - up)
    far = max(hops)
    dma = pltpu.SemaphoreType.DMA
    any_space = pl.BlockSpec(memory_space=pl.ANY)
    got = pl.pallas_call(
        functools.partial(kernel, (nb, nz, tok, slab, taps, pitch, cp, hops)),
        out_shape=jax.ShapeDtypeStruct((2 * cp, width), BF16),
        in_specs=[any_space] * 5 + [pl.BlockSpec(memory_space=pltpu.VMEM)],
        out_specs=pl.BlockSpec(memory_space=pltpu.VMEM),
        scratch_shapes=[
            pltpu.VMEM((2, xn, tok, LANES), BF16),
            pltpu.VMEM((2, xn, tok, LANES), BF16),
            pltpu.VMEM((2, xn, tok, LANES), BF16),
            pltpu.VMEM((2, xn, tok, LANES), BF16),
            pltpu.VMEM((xn, tok, LANES), BF16),
            pltpu.VMEM((taps, feats, width), BF16),
            pltpu.VMEM((nb * pitch, LANES), BF16),
            pltpu.VMEM((nb * pitch, 2 * LANES), BF16),
            pltpu.VMEM((2, 2 * pitch, LANES), BF16),
            pltpu.VMEM((pitch, feats), BF16),
            pltpu.VMEM((3, 4 * cp, feats), BF16),
            pltpu.VMEM((2, cp, feats), BF16),
            pltpu.VMEM((tok, feats), BF16),
            dma((xn,)), dma((2, xn)), dma((xn,)), dma((2, xn)), dma((xn,)), dma((2, xn)),
            dma((2, xn)), dma((xn,)),
            dma((2, parts)), dma((2, far, parts)), dma((2, parts)), dma((2, far, parts)),
            dma((2,)), dma((2,)), dma((2,)), pltpu.SemaphoreType.REGULAR,
            pltpu.VMEM((blocks, slab, width), BF16),
            pltpu.VMEM((2 * pitch, nb * pitch), F32),
            pltpu.VMEM((2 * pitch, nb * pitch), F32),
            dma((2,)), dma((2, far)),
        ],
        compiler_params=pltpu.CompilerParams(
            collective_id=0, has_side_effects=True, vmem_limit_bytes=60 * 1024 * 1024),
    )(queries, key_states, value_states, residual, conv_weight.reshape(9, slab, width), proj_weight)
    return got.reshape(ROWS, cp, width)[:, :COLS].reshape(1, tok, width)


def solution(mesh):
    return jax.shard_map(
        body,
        mesh=mesh,
        in_specs=(
            P(("groups", "batch"), "blk", None),
            P(("groups", "batch"), "blk", None),
            P(("groups", "batch"), "blk", None),
            P(("groups", "batch"), "blk", None),
            P(None, "batch"),
            P(None, None, "batch", None),
        ),
        out_specs=P(("groups", "batch"), "blk", None),
        check_vma=False,
    )
```
